32 devices in a mesh: snap: 2 (over core), shard: 16 (over z, y, x).
Axes of the slice: x: 2, y: 2, z: 4, core: 2. Of those that a mesh axis runs over, the one named last changes fastest.
Arguments:
- snapshots: float32 [32, 524288], P(('snap', 'shard')), may hold values from -6 to 6
- coefficients: float32 [32], P(('snap', 'shard')), may hold values from -1 to 1
Outputs:
- synthesized: float32 [524288], P('shard')
The draws below stay inside these ranges and needn't reach their ends.
All inputs are finite; a program needn't handle non-finite values.
Results may differ from the reference program's by a relative error of at most 0.000078.
Values sent between devices are 32-bit elements; how exact they have to be, the bound alone decides.
No kernel may reach another device: no remote copies, remote signals or barrier semaphores. Data moves between devices by JAX's collectives and lax.ppermute only.
A program may use at most 64 MiB of HBM per device.

```python
import jax
import jax.numpy as jnp
from jax import lax

PARAMS = 524288
SNAPSHOTS = 32


def raised(values, own_key, source, target, shards_of, factor):
    def block_of(dim):
        return (jnp.arange(values.shape[dim]) // (values.shape[dim] // shards_of)).reshape((-1,) + (1,) * (values.ndim - 1 - dim))

    one_side = jax.random.permutation(own_key, shards_of)[block_of(target)]
    second = (block_of(target) + shards_of // 2) % shards_of
    return jnp.where((block_of(source) == one_side) | (block_of(source) == second), factor * values, values)


def level_of(rng, shape, pieces, low, largest):
    level = 1.0
    for dim, blocks in pieces:
        heights = jax.random.uniform(jax.random.fold_in(jax.random.fold_in(rng, 6), dim), (blocks,), jnp.float32, low / len(pieces), largest / len(pieces))
        level = level * jnp.repeat(jnp.exp(heights), shape[dim] // blocks).reshape((-1,) + (1,) * (len(shape) - 1 - dim))
    return level


def scatter_about(key, shape, spread, limit, split=(), held_as=jnp.bfloat16):
    drawn = spread * jax.random.normal(key, shape, jnp.float32)
    if split:
        drawn = drawn * level_of(key, shape, split, -0.22, 0.18)
    return jnp.clip(drawn, -limit, limit).astype(held_as)


def gaussian_with(own_key, extent, deviation, bound, pieces, heavy, kind=jnp.bfloat16):
    result = deviation * jax.random.normal(own_key, extent, jnp.float32)
    if pieces:
        result = result * level_of(own_key, extent, pieces, -0.22, 0.18)
    return jnp.clip(raised(result, jax.random.fold_in(own_key, 3), *heavy), -bound, bound).astype(kind)


def setup_inputs(seed: int = 0) -> dict:
    key_list = jax.random.split(jax.random.key(seed), 3)
    return {
        "snapshots": gaussian_with(key_list[0], (SNAPSHOTS, PARAMS), 1.0, 6.0, ((0, 32),), (0, 1, 32, 2.75), jnp.float32),
        "coefficients": scatter_about(key_list[1], (SNAPSHOTS,), 0.0625, 1.0, ((0, 32),), jnp.float32),
    }


def reference(snapshots, coefficients):
    return jnp.dot(coefficients, snapshots, precision=lax.Precision.HIGHEST, preferred_element_type=jnp.float32)
```

```python
import jax
import jax.numpy as jnp
from jax import lax
from jax.sharding import PartitionSpec as P

LANES = 128


def halve(keep_src, axis_name, size, bit, index):
    pairs = [(i, i ^ (1 << bit)) for i in range(size)]
    mine = (index >> bit) & 1
    send = lax.dynamic_index_in_dim(keep_src, 1 - mine, 0, keepdims=False)
    keep = lax.dynamic_index_in_dim(keep_src, mine, 0, keepdims=False)
    return keep + lax.ppermute(send, axis_name, pairs)


def solution(mesh):
    snaps, shards = mesh.shape["snap"], mesh.shape["shard"]
    bits = shards.bit_length() - 1
    snap_bits = snaps.bit_length() - 1

    orders = [list(range(bits)), [1, 0] + list(range(2, bits))]
    colors = len(orders)

    def per_device(snapshots, coefficients):
        params = snapshots.shape[1]
        rows = params // shards // snaps // colors // LANES
        snap, shard = lax.axis_index("snap"), lax.axis_index("shard")
        weighted = jnp.sum(coefficients[:, None] * snapshots, axis=0)
        whole = weighted.reshape((2,) * bits + (2,) * snap_bits + (colors, rows, LANES))
        for bit in range(snap_bits):
            whole = halve(jnp.moveaxis(whole, bits + snap_bits - 1 - bit, 0), "snap", snaps, bit, snap)
        parts = []
        for color, order in enumerate(orders):
            part = lax.index_in_dim(whole, color, bits, keepdims=False)
            left = list(range(bits - 1, -1, -1))
            for bit in order:
                at = left.index(bit)
                part = halve(jnp.moveaxis(part, at, 0), "shard", shards, bit, shard)
                left.remove(bit)
            parts.append(part)
        own = jnp.stack(parts)
        return lax.all_gather(own, "snap", axis=0, tiled=True).reshape(-1)

    in_specs = (P(("snap", "shard"), None), P(("snap", "shard")))
    return jax.shard_map(per_device, mesh=mesh, in_specs=in_specs, out_specs=P("shard"), check_vma=False)
```

```python
import jax
import jax.numpy as jnp
from jax import lax
from jax.experimental import pallas as pl
from jax.experimental.pallas import tpu as pltpu
from jax.sharding import PartitionSpec as P

LANES = 128


def span(masks):
    offsets = [0]
    for mask in masks:
        offsets = offsets + [offset ^ mask for offset in offsets]
    return offsets


def phases_of(bits):
    rest = [(1 << b,) for b in range(min(4, bits), bits)]
    if bits < 4:
        return [(1 << b,) for b in range(bits)], [(1 << b,) for b in range(bits)]
    return [(1,), (2, 4), (8,)] + rest, [(2,), (1, 4), (8,)] + rest


def offsets_of(phases):
    offsets = [0]
    for masks in phases:
        offsets = [a ^ b for a in offsets for b in span(masks)]
    return offsets


def scaled_half(source, scale, half, order, shard, offsets):
    blocks, inner, _, rows, lanes = source.shape

    def kernel(half_ref, order_ref, shard_ref, scale_ref, source_ref, out_ref, sems):
        copies = []
        for k, (even, odd) in enumerate(zip(*offsets)):
            block = shard_ref[0] ^ jnp.where(order_ref[0] == 0, even, odd)
            copy = pltpu.make_async_copy(source_ref.at[block, :, half_ref[0]], out_ref.at[k], sems.at[k])
            copy.start()
            copies.append(copy)
        factor = scale_ref[0]
        for k, copy in enumerate(copies):
            copy.wait()
            out_ref[k] = out_ref[k] * factor

    smem = pl.BlockSpec(memory_space=pltpu.SMEM)
    return pl.pallas_call(
        kernel,
        out_shape=pltpu.VMEM((blocks, inner, rows, lanes), jnp.float32),
        in_specs=[smem, smem, smem, smem, pl.BlockSpec(memory_space=pltpu.HBM)],
        out_specs=pl.BlockSpec(memory_space=pltpu.VMEM),
        scratch_shapes=[pltpu.SemaphoreType.DMA((blocks,))],
    )(half.reshape(1), order.reshape(1), shard.reshape(1), scale, source)


def solution(mesh):
    snaps, shards = mesh.shape["snap"], mesh.shape["shard"]
    bits = shards.bit_length() - 1
    snap_bits = snaps.bit_length() - 1
    phases = phases_of(bits)
    offsets = [offsets_of(p) for p in phases]

    def per_device(snapshots, coefficients):
        params = snapshots.shape[1]
        rows = params // shards // snaps // LANES
        snap, shard = lax.axis_index("snap"), lax.axis_index("shard")
        source = snapshots.reshape(shards, -1, 2, rows, LANES)
        mine = snap & 1
        send = scaled_half(source, coefficients, 1 - mine, 1 - mine, shard, offsets)
        got = lax.ppermute(send, "snap", [(s, s ^ 1) for s in range(snaps)])
        part = scaled_half(source, coefficients, mine, mine, shard, offsets) + got
        for bit in range(1, snap_bits):
            mine = (snap >> bit) & 1
            part = part.reshape(shards, -1, 2, rows, LANES)
            send = lax.dynamic_index_in_dim(part, 1 - mine, 2, keepdims=False)
            keep = lax.dynamic_index_in_dim(part, mine, 2, keepdims=False)
            part = keep + lax.ppermute(send, "snap", [(s, s ^ (1 << bit)) for s in range(snaps)])
        part = part.reshape(shards, rows, LANES)
        for even, odd in zip(*phases):
            masks = list(zip(span(even), span(odd)))
            part = part.reshape(len(masks), -1, rows, LANES)
            total = part[0]
            for k in reversed(range(1, len(masks))):
                pairs = [
                    (s * shards + d, s * shards + (d ^ masks[k][s & 1]))
                    for s in range(snaps) for d in range(shards)
                ]
                total = total + lax.ppermute(part[k], ("snap", "shard"), pairs)
            part = total
        own = part.reshape(rows, LANES)
        for bit in range(snap_bits):
            mine = (snap >> bit) & 1
            got = lax.ppermute(own, "snap", [(s, s ^ (1 << bit)) for s in range(snaps)])
            own = jnp.stack([jnp.where(mine == 0, own, got), jnp.where(mine == 0, got, own)])
        return own.reshape(-1)

    in_specs = (P(("snap", "shard"), None), P(("snap", "shard")))
    return jax.shard_map(per_device, mesh=mesh, in_specs=in_specs, out_specs=P("shard"), check_vma=False)
```

```python
import jax
import jax.numpy as jnp
from jax import lax
from jax.experimental import pallas as pl
from jax.experimental.pallas import tpu as pltpu
from jax.sharding import PartitionSpec as P

LANES = 128


def span(masks):
    offsets = [0]
    for mask in masks:
        offsets = offsets + [offset ^ mask for offset in offsets]
    return offsets


def phases_of(bits):
    rest = [(1 << b,) for b in range(min(4, bits), bits)]
    if bits < 4:
        return [(1 << b,) for b in range(bits)], [(1 << b,) for b in range(bits)]
    return [(1,), (2, 4), (8,)] + rest, [(2,), (1, 4), (8,)] + rest


def offsets_of(phases):
    offsets = [0]
    for masks in phases:
        offsets = [a ^ b for a in offsets for b in span(masks)]
    return offsets


def scaled_half(source, scale, half, order, shard, offsets):
    _, inner, _, rows, lanes = source.shape
    blocks = len(offsets[0])

    def kernel(half_ref, order_ref, shard_ref, scale_ref, source_ref, out_ref, sems):
        copies = []
        for k, (even, odd) in enumerate(zip(*offsets)):
            block = shard_ref[0] ^ jnp.where(order_ref[0] == 0, even, odd)
            copy = pltpu.make_async_copy(source_ref.at[block, :, half_ref[0]], out_ref.at[k], sems.at[k])
            copy.start()
            copies.append(copy)
        factor = scale_ref[0]
        for k, copy in enumerate(copies):
            copy.wait()
            out_ref[k] = out_ref[k] * factor

    smem = pl.BlockSpec(memory_space=pltpu.SMEM)
    return pl.pallas_call(
        kernel,
        out_shape=pltpu.VMEM((blocks, inner, rows, lanes), jnp.float32),
        in_specs=[smem, smem, smem, smem, pl.BlockSpec(memory_space=pltpu.HBM)],
        out_specs=pl.BlockSpec(memory_space=pltpu.VMEM),
        scratch_shapes=[pltpu.SemaphoreType.DMA((blocks,))],
    )(half.reshape(1), order.reshape(1), shard.reshape(1), scale, source)


def solution(mesh):
    snaps, shards = mesh.shape["snap"], mesh.shape["shard"]
    bits = shards.bit_length() - 1
    snap_bits = snaps.bit_length() - 1
    phases = phases_of(bits)
    offsets = [offsets_of(p) for p in phases]
    first = [order[0][0] for order in phases]

    def per_device(snapshots, coefficients):
        params = snapshots.shape[1]
        rows = params // shards // snaps // LANES
        snap, shard = lax.axis_index("snap"), lax.axis_index("shard")
        source = snapshots.reshape(shards, -1, 2, rows, LANES)
        def snap_sum(scale, places):
            mine = snap & 1
            send = scaled_half(source, scale, 1 - mine, 1 - mine, shard, places)
            got = lax.ppermute(send, "snap", [(s, s ^ 1) for s in range(snaps)])
            part = scaled_half(source, scale, mine, mine, shard, places) + got
            for bit in range(1, snap_bits):
                mine = (snap >> bit) & 1
                part = part.reshape(len(places[0]), -1, 2, rows, LANES)
                send = lax.dynamic_index_in_dim(part, 1 - mine, 2, keepdims=False)
                keep = lax.dynamic_index_in_dim(part, mine, 2, keepdims=False)
                part = keep + lax.ppermute(send, "snap", [(s, s ^ (1 << bit)) for s in range(snaps)])
            return part.reshape(-1, rows, LANES)

        half = shards // 2
        sent = snap_sum(coefficients, [order[half:] for order in offsets])
        scale, sent = lax.optimization_barrier((coefficients, sent))
        pairs = [
            (s * shards + d, s * shards + (d ^ first[s & 1]))
            for s in range(snaps) for d in range(shards)
        ]
        came = lax.ppermute(sent, ("snap", "shard"), pairs)
        part = snap_sum(scale, [order[:half] for order in offsets]) + came
        for even, odd in zip(*(order[1:] for order in phases)):
            masks = list(zip(span(even), span(odd)))
            part = part.reshape(len(masks), -1, rows, LANES)
            total = part[0]
            for k in reversed(range(1, len(masks))):
                pairs = [
                    (s * shards + d, s * shards + (d ^ masks[k][s & 1]))
                    for s in range(snaps) for d in range(shards)
                ]
                total = total + lax.ppermute(part[k], ("snap", "shard"), pairs)
            part = total
        own = part.reshape(rows, LANES)
        for bit in range(snap_bits):
            mine = (snap >> bit) & 1
            got = lax.ppermute(own, "snap", [(s, s ^ (1 << bit)) for s in range(snaps)])
            own = jnp.stack([jnp.where(mine == 0, own, got), jnp.where(mine == 0, got, own)])
        return own.reshape(-1)

    in_specs = (P(("snap", "shard"), None), P(("snap", "shard")))
    return jax.shard_map(per_device, mesh=mesh, in_specs=in_specs, out_specs=P("shard"), check_vma=False)
```
